16 devices in a mesh: rep: 4 (over y, z, core), dp: 4 (over x).
Axes of the slice: x: 4, y: 2, z: 1, core: 2. Of those that a mesh axis runs over, the one named last changes fastest.
The devices are a block of a 4x4x8 slice.
Arguments:
- g_w_gate: bfloat16 [16, 2, 1024, 2816], P(('rep', 'dp')), parts along dimension 0
- g_w_up: bfloat16 [16, 2, 1024, 2816], P(('rep', 'dp')), parts along dimension 0
- g_w_down: bfloat16 [16, 2, 2816, 1024], P(('rep', 'dp')), parts along dimension 0
- w_gate: bfloat16 [2, 1024, 2816], replicated
- w_up: bfloat16 [2, 1024, 2816], replicated
- w_down: bfloat16 [2, 2816, 1024], replicated
- m_w_gate: float32 [2, 1024, 2816], P(None, 'dp')
- m_w_up: float32 [2, 1024, 2816], P(None, 'dp')
- m_w_down: float32 [2, 2816, 1024], P(None, 'dp')
- v_w_gate: float32 [2, 1024, 2816], P(None, 'dp')
- v_w_up: float32 [2, 1024, 2816], P(None, 'dp')
- v_w_down: float32 [2, 2816, 1024], P(None, 'dp')
Outputs:
- output 1: bfloat16 [8, 1024, 2816], P('rep'), parts along dimension 0
- output 2: bfloat16 [8, 1024, 2816], P('rep'), parts along dimension 0
- output 3: bfloat16 [8, 2816, 1024], P('rep'), parts along dimension 0
- output 4: float32 [8, 1024, 2816], P('rep', 'dp'), parts along dimension 0
- output 5: float32 [8, 1024, 2816], P('rep', 'dp'), parts along dimension 0
- output 6: float32 [8, 2816, 1024], P('rep', 'dp'), parts along dimension 0
- output 7: float32 [8, 1024, 2816], P('rep', 'dp'), parts along dimension 0
- output 8: float32 [8, 1024, 2816], P('rep', 'dp'), parts along dimension 0
- output 9: float32 [8, 2816, 1024], P('rep', 'dp'), parts along dimension 0
There are 4 independent parts. The reference program is written for one: setup_inputs(seed, part) draws one part's arguments, and reference() takes and returns one part's arrays. A program takes and returns all parts, laid end to end along the dimension named above; an argument that names none is the same for every part.
All inputs are finite; a program needn't handle non-finite values.
Results may differ from the reference program's by a relative error of at most 0.022.
Values are sent between devices in bfloat16 or wider.
A program may use at most 768 MiB of HBM per device.

```python
import jax
import jax.numpy as jnp
from jax import lax

DEVICES = 4
D = 1024
FF = 2816
LAYERS = 2
NAMES = ("w_gate", "w_up", "w_down")
SHAPES = {"w_gate": (LAYERS, D, FF), "w_up": (LAYERS, D, FF), "w_down": (LAYERS, FF, D)}


def setup_inputs(seed: int = 0, part: int = 0) -> dict:
    kz, *keys = jax.random.split(jax.random.key(seed), 1 + 5 * len(NAMES))
    loud = 2.0 ** jax.random.uniform(kz, (), jnp.float32, -1.0, 1.0)
    drawn = {}
    for name, key, both in zip(NAMES, keys[:3], keys[3:6], strict=True):
        own = jax.random.normal(jax.random.fold_in(key, part), (DEVICES, *SHAPES[name]), jnp.float32)
        shared = jax.random.normal(jax.random.fold_in(both, part), SHAPES[name], jnp.float32)
        drawn["g_" + name] = (loud * (0.7 * shared / DEVICES + 0.7 * own * DEVICES**-0.5)).astype(jnp.bfloat16)
    for name, key in zip(NAMES, keys[6:9], strict=True):
        drawn[name] = (jax.random.normal(key, SHAPES[name], jnp.float32) * SHAPES[name][1] ** -0.5).astype(jnp.bfloat16)
    for name, key in zip(NAMES, keys[9:12], strict=True):
        drawn["m_" + name] = loud * 0.5 * jax.random.normal(key, SHAPES[name], jnp.float32)
    for name, key in zip(NAMES, keys[12:15], strict=True):
        drawn["v_" + name] = loud * loud * jax.random.uniform(key, SHAPES[name], jnp.float32, 0.5, 1.5)
    return drawn


def adamw(w, m, v, g):
    m = 0.9 * m + 0.1 * g
    v = 0.95 * v + 0.05 * g * g
    step = m * lax.rsqrt(v + 1e-8) + 0.1 * w
    return (w - 0.02 * step).astype(jnp.bfloat16), m, v


def reference(g_w_gate, g_w_up, g_w_down, w_gate, w_up, w_down, m_w_gate, m_w_up, m_w_down, v_w_gate, v_w_up, v_w_down):
    def total(terms):
        return lax.scan(lambda so_far, term: (so_far + term.astype(jnp.float32), None), jnp.zeros(terms.shape[1:], jnp.float32), terms)[0]

    gradients = [total(terms).astype(jnp.bfloat16).astype(jnp.float32) for terms in (g_w_gate, g_w_up, g_w_down)]
    new = [
        adamw(w.astype(jnp.float32), m, v, g)
        for w, m, v, g in zip((w_gate, w_up, w_down), (m_w_gate, m_w_up, m_w_down), (v_w_gate, v_w_up, v_w_down), gradients, strict=True)
    ]
    return tuple(one[which] for which in range(3) for one in new)
```

```python
import jax
import jax.numpy as jnp
from jax import lax
from jax.experimental import pallas as pl
from jax.experimental.pallas import tpu as pltpu
from jax.sharding import PartitionSpec as P


def adamw(w, m, v, g):
    m = 0.9 * m + 0.1 * g
    v = 0.95 * v + 0.05 * g * g
    step = m * lax.rsqrt(v + 1e-8) + 0.1 * w
    return (w - 0.02 * step).astype(jnp.bfloat16), m, v


def fresh(shape, dtype):
    return pl.pallas_call(
        lambda ref: None,
        out_shape=jax.ShapeDtypeStruct(shape, dtype),
        out_specs=pl.BlockSpec(memory_space=pl.ANY),
        compiler_params=pltpu.CompilerParams(has_side_effects=True),
    )()


def solution(mesh):
    n = mesh.shape["dp"]
    assert n == 4
    to_right = [(i, (i + 1) % n) for i in range(n)]
    to_left = [(i, (i - 1) % n) for i in range(n)]

    def send(x, way, name):
        with jax.named_scope(name):
            return lax.ppermute(x, "dp", to_right if way == "r" else to_left)

    def step(*arrays):
        terms, weights, m, v = (arrays[i : i + 3] for i in (0, 3, 6, 9))
        me = lax.axis_index("dp")
        right, far, left = ((me + k) % n for k in (1, 2, 3))
        layers = weights[0].shape[0]
        f32 = jnp.float32
        whole = [fresh(w.shape, w.dtype) for w in weights]
        sums = {}
        for i in range(3):
            rows = m[i].shape[1]
            half = rows // 2
            cols = m[i].shape[2]

            def part(x, layer, block, h, lead=()):
                at = (layer, block * rows + h * half, 0)
                return lax.dynamic_slice(x, at, (1, half, cols))[0]

            for layer in range(layers):
                tag = f"{i}_{layer}"
                term = terms[i][0]
                rounded = lambda x: x.astype(jnp.bfloat16)
                ar = send(part(term, layer, far, 0), "r", f"ar{tag}")
                al = send(part(term, layer, far, 1), "l", f"al{tag}")
                rawr = send(part(term, layer, right, 1), "r", f"rawr{tag}")
                rawl = send(part(term, layer, left, 0), "l", f"rawl{tag}")
                br = send(rounded(ar.astype(f32) + part(term, layer, right, 0).astype(f32)), "r", f"br{tag}")
                bl = send(rounded(al.astype(f32) + part(term, layer, left, 1).astype(f32)), "l", f"bl{tag}")
                new = []
                for h, (one, two) in enumerate(((br, rawl), (rawr, bl))):
                    g = part(term, layer, me, h).astype(f32) + one.astype(f32) + two.astype(f32)
                    g = lax.reduce_precision(g, 8, 7)
                    sums[i, layer, h] = rounded(g)
                    own = part(weights[i], layer, me, h).astype(f32)
                    rs = slice(h * half, (h + 1) * half)
                    new.append(adamw(own, m[i][layer, rs], v[i][layer, rs], g)[0])
                cr = [send(new[h], "r", f"cr{h}{tag}") for h in range(2)]
                cl = [send(new[h], "l", f"cl{h}{tag}") for h in (1, 0)][::-1]
                dr = send(cr[0], "r", f"dr{tag}")
                dl = send(cl[1], "l", f"dl{tag}")

                def put(x, block, h):
                    at = (layer, block * rows + h * half, 0)
                    whole[i] = lax.dynamic_update_slice(whole[i], x[None], at)

                for h in range(2):
                    put(new[h], me, h)
                for h in range(2):
                    put(cr[h], left, h)
                    put(cl[h], right, h)
                put(dr, far, 0)
                put(dl, far, 1)
        moments = []
        for i in range(3):
            g = jnp.stack([jnp.concatenate([sums[i, layer, h] for h in range(2)]) for layer in range(layers)])
            g = g.astype(f32)
            moments.append((0.9 * m[i] + 0.1 * g, 0.95 * v[i] + 0.05 * g * g))
        return (*whole, *(one[0] for one in moments), *(one[1] for one in moments))

    all_of, cut = P(None, None, None), P(None, "dp", None)
    return jax.shard_map(
        step,
        mesh=mesh,
        in_specs=(P(("rep", "dp"), None, None, None),) * 3 + (all_of,) * 3 + (cut,) * 6,
        out_specs=(P("rep", None, None),) * 3 + (P("rep", "dp", None),) * 6,
        check_vma=False,
    )
```
